32 devices in a mesh: blk: 16 (over z, x, core), dp: 2 (over y).
Axes of the slice: x: 2, y: 2, z: 4, core: 2. Of those that a mesh axis runs over, the one named last changes fastest.
Arguments:
- inputs: bfloat16 [4096, 1024], P(('blk', 'dp')), may hold values from -6 to 6
- cotangent: bfloat16 [4096, 1024], P(('blk', 'dp')), may hold values from -2.5 to 2.5
- task_ids: int32 [4096], P(('blk', 'dp')), may hold values from 0 to 3
- group_counts: int32 [32, 8], P(('blk', 'dp')), may hold values from 1 to 16, as said below
- task_gate: float32 [4, 16], replicated, may hold values from 0.25 to 2
- w_in: bfloat16 [16, 1024, 2048], P('blk'), may hold values from -0.1875 to 0.1875
- w_out: bfloat16 [16, 2048, 1024], P('blk'), may hold values from -0.125 to 0.125
Outputs:
- input_grad: float32 [4096, 1024], P(('blk', 'dp'))
- grad_in: float32 [16, 1024, 2048], P('blk', 'dp')
- grad_out: float32 [16, 2048, 1024], P('blk', 'dp')
The draws below stay inside these ranges and needn't reach their ends.
Inputs may be any that keep to these rules, and one draw needn't show every extreme that they name: `group_counts`: in every draw one group has all 16 slots live on every device; the others vary from device to device.
All inputs are finite; a program needn't handle non-finite values.
Results may differ from the reference program's by a relative error of at most 0.0042.
Values may be sent and summed in bfloat16 or wider, within the bound.
No kernel may reach another device: no remote copies, remote signals or barrier semaphores. Data moves between devices by JAX's collectives and lax.ppermute only.
A program may use at most 128 MiB of HBM per device.

```python
import math
import jax
import jax.numpy as jnp
from jax import lax

D = 1024
HW = 2048
GROUPS = 8
TASKS = 4
CAP = 16
EXPERTS = 16
SOURCES = 32
SAMPLES = 4096


def draw_group_counts(key, part):
    key_level = jax.random.fold_in(key, 11)
    key_raw = jax.random.fold_in(key, 12)
    key_full = jax.random.fold_in(key, 13)
    level = jax.random.randint(key_level, (GROUPS,), max(1, CAP // 4), CAP + 1)
    raw_values = jax.random.randint(key_raw, (SOURCES, GROUPS), 0, 1 << 20)
    counts = 1 + raw_values % level[None, :]
    full_group = jax.random.randint(key_full, (), 0, GROUPS)
    filled = jnp.where(jnp.arange(GROUPS)[None, :] == full_group, CAP, counts)
    return filled.astype(jnp.int32)


def with_ends(entries, rng, smallest, high):
    longest = entries.shape.index(max(entries.shape))
    spots = []
    for shift in (0, 1):
        where = [jax.random.randint(jax.random.fold_in(rng, axis), (), 0, length) for axis, length in enumerate(entries.shape)]
        where[longest] = (where[longest] + shift) % entries.shape[longest]
        spots.append(tuple(where))
    return entries.at[spots[0]].set(smallest).at[spots[1]].set(high)


def level_of(stream_key, dims, cuts, least, high):
    loudness = 1.0
    for dim, shards_of in cuts:
        steps = jax.random.uniform(jax.random.fold_in(jax.random.fold_in(stream_key, 6), dim), (shards_of,), jnp.float32, least / len(cuts), high / len(cuts))
        loudness = loudness * jnp.repeat(jnp.exp(steps), dims[dim] // shards_of).reshape((-1,) + (1,) * (len(dims) - 1 - dim))
    return loudness


def noise(key, dims, deviation, limit, shards=(), kind=jnp.bfloat16):
    level = level_of(key, dims, shards, -0.22, 0.18) if shards else 1.0
    drawn = jax.random.normal(key, dims, jnp.float32) * deviation * level
    return jnp.minimum(jnp.maximum(drawn, -limit), limit).astype(kind)


def setup_inputs(seed: int = 0) -> dict:
    key_list = jax.random.split(jax.random.key(seed), 8)
    return {
        "inputs": noise(key_list[0], (SAMPLES, D), 1.0, 6.0, ((0, 32),)),
        "cotangent": noise(key_list[1], (SAMPLES, D), 0.35, 2.5, ((0, 32),)),
        "task_ids": with_ends(jax.random.randint(key_list[2], (SAMPLES,), 0, TASKS), jax.random.fold_in(key_list[2], 1), 0, TASKS - 1).astype(jnp.int32),
        "group_counts": draw_group_counts(jax.random.fold_in(key_list[7], 71), 0),
        "task_gate": jnp.clip(jnp.exp(jax.random.uniform(key_list[4], (TASKS, EXPERTS), jnp.float32, math.log(0.25), math.log(2.0))), 0.25, 2.0),
        "w_in": noise(key_list[5], (EXPERTS, D, HW), D ** -0.5, 0.1875, ((0, 16),)),
        "w_out": noise(key_list[6], (EXPERTS, HW, D), HW ** -0.5, 0.125, ((0, 16),)),
    }


grad_scale = 0.0625


def reference(inputs, cotangent, task_ids, group_counts, task_gate, w_in, w_out):
    inputs_four = inputs.reshape(SOURCES, GROUPS, CAP, D)
    cot_four = cotangent.reshape(SOURCES, GROUPS, CAP, D)
    task_three = task_ids.reshape(SOURCES, GROUPS, CAP)
    slot_index = jnp.arange(CAP, dtype=jnp.int32)
    live_three = slot_index[None, None, :] < group_counts[:, :, None]

    def per_expert(accum, expert):
        group = (expert % GROUPS).astype(jnp.int32)
        x_rows = lax.dynamic_index_in_dim(inputs_four, group, 1, keepdims=False).reshape(SOURCES * CAP, D)
        cot_rows = lax.dynamic_index_in_dim(cot_four, group, 1, keepdims=False).reshape(SOURCES * CAP, D)
        task_rows = lax.dynamic_index_in_dim(task_three, group, 1, keepdims=False).reshape(SOURCES * CAP)
        live_rows = lax.dynamic_index_in_dim(live_three, group, 1, keepdims=False).reshape(SOURCES * CAP)
        column = lax.dynamic_index_in_dim(task_gate, expert.astype(jnp.int32), 1, keepdims=False)
        row_gate = jnp.where(live_rows, column[task_rows], jnp.zeros((), task_gate.dtype)).astype(jnp.float32)
        first_weight = lax.dynamic_index_in_dim(w_in, expert.astype(jnp.int32), 0, keepdims=False)
        second_weight = lax.dynamic_index_in_dim(w_out, expert.astype(jnp.int32), 0, keepdims=False)
        pre_act = jnp.dot(x_rows, first_weight, preferred_element_type=jnp.float32)
        sigmoid_act = jax.nn.sigmoid(pre_act)
        hidden = (pre_act * sigmoid_act).astype(jnp.bfloat16)
        scaled_cot = (row_gate[:, None] * cot_rows.astype(jnp.float32)).astype(jnp.bfloat16)
        hidden_cot = jnp.dot(scaled_cot, second_weight.T, preferred_element_type=jnp.float32)
        pre_cot = (hidden_cot * sigmoid_act * (1.0 + pre_act * (1.0 - sigmoid_act))).astype(jnp.bfloat16)
        grad_second = jnp.dot(hidden.T, scaled_cot, preferred_element_type=jnp.float32) * grad_scale
        grad_first = jnp.dot(x_rows.T, pre_cot, preferred_element_type=jnp.float32) * grad_scale
        row_grad = jnp.dot(pre_cot, first_weight.T, preferred_element_type=jnp.float32)
        current = lax.dynamic_index_in_dim(accum, group, 1, keepdims=False)
        accum = lax.dynamic_update_index_in_dim(accum, current + row_grad.reshape(SOURCES, CAP, D), group, 1)
        return accum, (grad_first, grad_second)

    start = jnp.zeros((SOURCES, GROUPS, CAP, D), jnp.float32)
    accum, stacked = lax.scan(per_expert, start, jnp.arange(EXPERTS, dtype=jnp.int32))
    return accum.reshape(SAMPLES, D), stacked[0], stacked[1]
```

```python
import jax
import jax.numpy as jnp
from jax import lax
from jax.sharding import PartitionSpec as P

grad_scale = 0.0625
tag_lanes = 128


def contract(left, right, left_dim, right_dim):
    return lax.dot_general(
        left, right, (((left_dim,), (right_dim,)), ((), ())), preferred_element_type=jnp.float32
    )


def hidden_parts(packed, first_weight, second_weight, gate_column):
    model_width = first_weight.shape[0]
    x_rows = packed[:, :model_width]
    cot_rows = packed[:, model_width : 2 * model_width]
    tags = packed[:, 2 * model_width : 2 * model_width + 1].astype(jnp.float32)
    row_gate = jnp.zeros_like(tags)
    for task in range(gate_column.shape[0]):
        row_gate = jnp.where(tags == task, gate_column[task], row_gate)
    pre_act = contract(x_rows, first_weight, 1, 0)
    sigmoid_act = jax.nn.sigmoid(pre_act)
    hidden = (pre_act * sigmoid_act).astype(jnp.bfloat16)
    scaled_cot = (row_gate * cot_rows.astype(jnp.float32)).astype(jnp.bfloat16)
    hidden_cot = contract(scaled_cot, second_weight, 1, 1)
    pre_cot = hidden_cot * (sigmoid_act * (1.0 + pre_act * (1.0 - sigmoid_act)))
    return x_rows, hidden, scaled_cot, pre_cot.astype(jnp.bfloat16)


def on_device(inputs, cotangent, task_ids, group_counts, task_gate, w_in, w_out):
    groups = group_counts.shape[1]
    model_width = inputs.shape[1]
    capacity = inputs.shape[0] // groups
    task_count = task_gate.shape[0]
    expert_count = lax.axis_size("blk")
    expert_index = lax.axis_index("blk")
    half_count = lax.axis_size("dp")
    half_index = lax.axis_index("dp")
    repeats = expert_count // groups
    first_weight = w_in[0]
    second_weight = w_out[0]
    expert_match = jnp.arange(task_gate.shape[1], dtype=jnp.int32) == expert_index
    gate_column = jnp.sum(jnp.where(expert_match[None, :], task_gate, 0.0), axis=1)
    slot_index = jnp.arange(capacity, dtype=jnp.int32)
    live_slots = slot_index[None, :] < group_counts[0][:, None]
    tags = jnp.where(live_slots, task_ids.reshape(groups, capacity), task_count)
    tag_columns = jnp.broadcast_to(
        tags.reshape(groups * capacity, 1).astype(jnp.bfloat16), (groups * capacity, tag_lanes)
    )
    packed = jnp.concatenate([inputs, cotangent, tag_columns], axis=1)
    packed_width = packed.shape[1]
    outgoing = jnp.broadcast_to(
        packed.reshape(1, groups, capacity, packed_width),
        (repeats, groups, capacity, packed_width),
    ).reshape(expert_count, capacity, packed_width)
    own_rows = lax.all_to_all(outgoing, "blk", 0, 0).reshape(
        expert_count * capacity, packed_width
    )
    row_count = own_rows.shape[0]
    pieces = 2
    piece_rows = row_count // pieces
    other_rows = []
    for hop in range(1, half_count):
        ring = [(i, (i + hop) % half_count) for i in range(half_count)]
        for piece in range(pieces):
            part = own_rows[piece * piece_rows : (piece + 1) * piece_rows]
            other_rows.append(lax.ppermute(part, "dp", ring))
    own = hidden_parts(own_rows, first_weight, second_weight, gate_column)
    row_grads = contract(own[3], first_weight, 1, 1).astype(jnp.bfloat16)
    returned = lax.all_to_all(
        row_grads.reshape(expert_count, capacity, model_width), "blk", 0, 0
    )
    parts = [own] + [
        hidden_parts(rows, first_weight, second_weight, gate_column) for rows in other_rows
    ]
    first_span = model_width // half_count
    second_span = first_weight.shape[1] // half_count
    all_x = jnp.concatenate([part[0] for part in parts])
    all_hidden = jnp.concatenate([part[1] for part in parts])
    all_scaled = jnp.concatenate([part[2] for part in parts])
    all_pre = jnp.concatenate([part[3] for part in parts])
    left_first = lax.dynamic_slice_in_dim(all_x, half_index * first_span, first_span, 1)
    left_second = lax.dynamic_slice_in_dim(all_hidden, half_index * second_span, second_span, 1)
    grad_first = contract(left_first, all_pre, 0, 0) * grad_scale
    grad_second = contract(left_second, all_scaled, 0, 0) * grad_scale
    input_home = jnp.sum(
        returned.reshape(repeats, groups * capacity, model_width).astype(jnp.float32), axis=0
    )
    return (input_home, grad_first[None], grad_second[None])


def solution(mesh):
    in_specs = (
        P(("blk", "dp"), None),
        P(("blk", "dp"), None),
        P(("blk", "dp")),
        P(("blk", "dp"), None),
        P(),
        P("blk", None, None),
        P("blk", None, None),
    )
    out_specs = (P(("blk", "dp"), None), P("blk", "dp", None), P("blk", "dp", None))
    return jax.shard_map(
        on_device, mesh=mesh, in_specs=in_specs, out_specs=out_specs, check_vma=False
    )
```

```python
import functools

import jax
import jax.numpy as jnp
from jax import lax
from jax.experimental import pallas as pl
from jax.experimental.pallas import tpu as pltpu
from jax.sharding import Mesh
from jax.sharding import PartitionSpec as P

grad_scale = 0.0625
lanes = 128
far_pieces = 2


def contract(left, right, left_dim, right_dim):
    return lax.dot_general(
        left, right, (((left_dim,), (right_dim,)), ((), ())), preferred_element_type=jnp.float32
    )


def pack_kernel(repeats, groups, capacity, ids, counts, table, x_ref, cot_ref, *outs):
    near_ref, far_refs = outs[0], outs[1:]
    model_width = x_ref.shape[1]
    own_repeat = lax.axis_index("rep")
    own_group = lax.axis_index("grp")
    row = lax.broadcasted_iota(jnp.int32, (capacity, lanes), 0)

    def fill(block_refs, group, expert):
        start = pl.multiple_of(group * capacity, capacity)
        live = counts[0, group]
        gate = jnp.zeros((capacity, lanes), jnp.float32)
        for slot in range(capacity):
            value = table[ids[start + slot], expert]
            gate = jnp.where(row == slot, jnp.where(slot < live, value, 0.0), gate)
        rows = pl.ds(start, capacity)
        for ref in block_refs:
            ref[:, :model_width] = x_ref[rows, :]
        for column in range(0, model_width, lanes):
            part = cot_ref[rows, column : column + lanes].astype(jnp.float32) * gate
            part = part.astype(jnp.bfloat16)
            for ref in block_refs:
                ref[:, model_width + column : model_width + column + lanes] = part

    for hop in range(1, repeats):
        for step in range(groups):
            group = lax.rem(own_group + step, groups)
            expert = lax.rem(own_repeat + hop, repeats) * groups + group
            fill([far_refs[(hop - 1) * groups + step]], group, expert)
    for group in range(groups):
        fill(
            [near_ref.at[half, group] for half in range(near_ref.shape[0])],
            group,
            own_repeat * groups + group,
        )


def pack_blocks(sizes, task_ids, group_counts, task_gate, inputs, cotangent):
    repeats, groups, halves, capacity = sizes
    width = 2 * inputs.shape[1]
    far_count = (repeats - 1) * groups
    smem = pl.BlockSpec(memory_space=pltpu.SMEM)
    vmem = pl.BlockSpec(memory_space=pltpu.VMEM)
    out_shape = [jax.ShapeDtypeStruct((halves, groups, capacity, width), jnp.bfloat16)]
    out_shape += [jax.ShapeDtypeStruct((capacity, width), jnp.bfloat16)] * far_count
    outs = pl.pallas_call(
        functools.partial(pack_kernel, repeats, groups, capacity),
        out_shape=out_shape,
        in_specs=[smem, smem, smem, vmem, vmem],
        out_specs=[vmem] * len(out_shape),
        name="pack_blocks",
    )(task_ids, group_counts, task_gate, inputs, cotangent)
    return outs[0], outs[1:]


def hidden_parts(packed, first_weight, second_weight):
    model_width = first_weight.shape[0]
    x_rows = packed[:, :model_width]
    scaled_cot = packed[:, model_width:]
    pre_act = contract(x_rows, first_weight, 1, 0)
    sigmoid_act = jax.nn.sigmoid(pre_act)
    hidden = (pre_act * sigmoid_act).astype(jnp.bfloat16)
    hidden_cot = contract(scaled_cot, second_weight, 1, 1)
    pre_cot = hidden_cot * (sigmoid_act * (1.0 + pre_act * (1.0 - sigmoid_act)))
    return x_rows, hidden, scaled_cot, pre_cot.astype(jnp.bfloat16)


def on_device(inputs, cotangent, task_ids, group_counts, task_gate, w_in, w_out):
    groups = group_counts.shape[1]
    model_width = inputs.shape[1]
    capacity = inputs.shape[0] // groups
    repeats = lax.axis_size("rep")
    halves = lax.axis_size("dp")
    half_index = lax.axis_index("dp")
    first_weight = w_in[0]
    second_weight = w_out[0]
    near, far = pack_blocks(
        (repeats, groups, halves, capacity), task_ids, group_counts, task_gate, inputs, cotangent
    )
    width = near.shape[-1]

    def ring(hop, step):
        pairs = []
        for source in range(repeats * groups):
            repeat, group = divmod(source, groups)
            target = ((repeat + hop) % repeats) * groups + (group + step) % groups
            pairs.append((source, target))
        return pairs

    far_blocks = [
        [
            lax.ppermute(far[(hop - 1) * groups + step], ("rep", "grp"), ring(hop, step))
            for step in range(groups)
        ]
        for hop in range(1, repeats)
    ]
    near_rows = lax.all_to_all(
        near.reshape(halves * groups, capacity, width), ("dp", "grp"), 0, 0
    ).reshape(halves, groups * capacity, width)

    per_piece = groups // far_pieces
    back = [[] for _ in range(1, repeats)]
    parts = []
    other_rows = []
    for hop in range(1, repeats):
        for piece in range(far_pieces):
            blocks = far_blocks[hop - 1][piece * per_piece : (piece + 1) * per_piece]
            rows = jnp.concatenate(blocks)
            for turn in range(1, halves):
                pairs = [(i, (i + turn) % halves) for i in range(halves)]
                other_rows.append(lax.ppermute(rows, "dp", pairs))
            part = hidden_parts(rows, first_weight, second_weight)
            parts.append(part)
            row_grads = contract(part[3], first_weight, 1, 1).astype(jnp.bfloat16)
            pairs = [(i, (i - hop) % repeats) for i in range(repeats)]
            back[hop - 1].append(lax.ppermute(row_grads, "rep", pairs))

    near_part = hidden_parts(
        near_rows.reshape(halves * groups * capacity, width), first_weight, second_weight
    )
    parts.append(near_part)
    own_pre = lax.dynamic_slice_in_dim(
        near_part[3], half_index * groups * capacity, groups * capacity, 0
    )
    near_grads = contract(own_pre, first_weight, 1, 1).reshape(groups, capacity, model_width)
    own_group = lax.axis_index("grp")
    slots = []
    for step in range(groups):
        piece, place = divmod(step, per_piece)
        source = (own_group - step) % groups
        total = lax.dynamic_index_in_dim(near_grads, source, 0, keepdims=False)
        for hop in range(1, repeats):
            block = back[hop - 1][piece][place * capacity : (place + 1) * capacity]
            total = total + block.astype(jnp.float32)
        slots.append(total)
    home = jnp.zeros((groups, capacity, model_width), jnp.bfloat16)
    for step in range(groups):
        source = (own_group - step) % groups
        home = lax.dynamic_update_index_in_dim(
            home, slots[step].astype(jnp.bfloat16), source, 0
        )
    returned = lax.all_to_all(home, "grp", 0, 0)
    if other_rows:
        parts.append(hidden_parts(jnp.concatenate(other_rows), first_weight, second_weight))
    first_span = model_width // halves
    second_span = first_weight.shape[1] // halves
    all_x, all_hidden, all_scaled, all_pre = (
        jnp.concatenate([part[i] for part in parts]) for i in range(4)
    )
    left_first = lax.dynamic_slice_in_dim(all_x, half_index * first_span, first_span, 1)
    left_second = lax.dynamic_slice_in_dim(all_hidden, half_index * second_span, second_span, 1)
    grad_first = contract(left_first, all_pre, 0, 0) * grad_scale
    grad_second = contract(left_second, all_scaled, 0, 0) * grad_scale
    input_home = returned.astype(jnp.float32).reshape(groups * capacity, model_width)
    return (input_home, grad_first[None], grad_second[None])


def solution(mesh):
    def step(inputs, cotangent, task_ids, group_counts, task_gate, w_in, w_out):
        groups = group_counts.shape[1]
        halves = mesh.shape["dp"]
        repeats = mesh.shape["blk"] // groups
        fine = Mesh(mesh.devices.reshape(repeats, groups, halves), ("rep", "grp", "dp"))
        rows = P(("rep", "grp", "dp"))
        expert = P(("rep", "grp"))
        split = P(("rep", "grp"), "dp")
        return jax.shard_map(
            on_device,
            mesh=fine,
            in_specs=(rows, rows, rows, rows, P(), expert, expert),
            out_specs=(rows, split, split),
            check_vma=False,
        )(inputs, cotangent, task_ids, group_counts, task_gate, w_in, w_out)

    return step
```

```python
import functools

import jax
import jax.numpy as jnp
from jax import lax
from jax.experimental import pallas as pl
from jax.experimental.pallas import tpu as pltpu
from jax.sharding import Mesh
from jax.sharding import PartitionSpec as P

grad_scale = 0.0625
lanes = 128
hidden_tile = 512
hidden_chunk = 256


smem_spec = pl.BlockSpec(memory_space=pltpu.SMEM)
vmem_spec = pl.BlockSpec(memory_space=pltpu.VMEM)


def contract(left, right, left_dim, right_dim):
    return lax.dot_general(
        left, right, (((left_dim,), (right_dim,)), ((), ())), preferred_element_type=jnp.float32
    )


def partner_of(group, step, groups):
    if groups & (groups - 1) == 0:
        return group ^ step
    return (group + step) % groups


def partner(group, step, groups, sign):
    if groups & (groups - 1) == 0:
        return group ^ step
    return lax.rem(group + sign * step + groups, groups)


def pack_kernel(repeats, groups, capacity, ids, counts, table, x_ref, cot_ref, *outs):
    all_ref, near_refs = outs[0], outs[1:]
    model_width = x_ref.shape[1]
    own_repeat = lax.axis_index("rep")
    own_group = lax.axis_index("grp")
    row = lax.broadcasted_iota(jnp.int32, (capacity, lanes), 0)

    def fill(block_refs, group, expert):
        start = pl.multiple_of(group * capacity, capacity)
        live = counts[0, group]
        gate = jnp.zeros((capacity, lanes), jnp.float32)
        for slot in range(capacity):
            value = table[ids[start + slot], expert]
            gate = jnp.where(row == slot, jnp.where(slot < live, value, 0.0), gate)
        rows = pl.ds(start, capacity)
        for ref in block_refs:
            ref[:, :model_width] = x_ref[rows, :]
        for column in range(0, model_width, lanes):
            part = cot_ref[rows, column : column + lanes].astype(jnp.float32) * gate
            part = part.astype(jnp.bfloat16)
            for ref in block_refs:
                ref[:, model_width + column : model_width + column + lanes] = part

    for hop in range(repeats):
        repeat = lax.rem(own_repeat + hop, repeats)
        for step in range(groups):
            group = partner(own_group, step, groups, 1)
            expert = repeat * groups + group
            block_refs = [all_ref.at[expert]]
            if hop == 0 and near_refs:
                block_refs.append(near_refs[step])
            fill(block_refs, group, expert)


def pack_blocks(sizes, task_ids, group_counts, task_gate, inputs, cotangent):
    repeats, groups, halves, capacity = sizes
    width = 2 * inputs.shape[1]
    near_count = groups if halves > 1 else 0
    out_shape = [jax.ShapeDtypeStruct((repeats * groups, capacity, width), jnp.bfloat16)]
    out_shape += [jax.ShapeDtypeStruct((capacity, width), jnp.bfloat16)] * near_count
    outs = pl.pallas_call(
        functools.partial(pack_kernel, repeats, groups, capacity),
        out_shape=out_shape,
        in_specs=[smem_spec, smem_spec, smem_spec, vmem_spec, vmem_spec],
        out_specs=[vmem_spec] * len(out_shape),
        name="pack_blocks",
    )(task_ids, group_counts, task_gate, inputs, cotangent)
    return outs[0], outs[1:]


def hidden_kernel(rows_ref, first_ref, second_ref, act_ref, pre_ref, *grads):
    model_width, tile = first_ref.shape
    x_rows = rows_ref[:, :model_width]
    scaled_cot = rows_ref[:, model_width:]
    part = None
    for start in range(0, tile, hidden_chunk):
        columns = slice(start, start + hidden_chunk)
        first = first_ref[:, columns]
        pre_act = contract(x_rows, first, 1, 0)
        sigmoid_act = 1.0 / (1.0 + jnp.exp(-pre_act))
        value = pre_act * sigmoid_act
        act_ref[:, columns] = value.astype(jnp.bfloat16)
        slope = sigmoid_act * (1.0 + pre_act - value)
        hidden_cot = contract(scaled_cot, second_ref[columns, :], 1, 1)
        pre_cot = (hidden_cot * slope).astype(jnp.bfloat16)
        pre_ref[:, columns] = pre_cot
        if grads:
            piece = contract(pre_cot, first, 1, 1)
            part = piece if part is None else part + piece
    if grads:
        grad_ref, total = grads
        step = pl.program_id(0)

        @pl.when(step == 0)
        def _():
            total[...] = part

        @pl.when(step > 0)
        def _():
            total[...] += part

        @pl.when(step == pl.num_programs(0) - 1)
        def _():
            grad_ref[...] = total[...].astype(grad_ref.dtype)


def hidden_parts(rows, first_weight, second_weight, with_grads):
    row_count, width = rows.shape
    model_width, hidden_width = first_weight.shape
    tile = hidden_tile
    out_shape = [jax.ShapeDtypeStruct((row_count, hidden_width), jnp.bfloat16)] * 2
    out_specs = [pl.BlockSpec((row_count, tile), lambda i: (0, i))] * 2
    scratch = []
    if with_grads:
        out_shape.append(jax.ShapeDtypeStruct((row_count, model_width), jnp.bfloat16))
        out_specs.append(pl.BlockSpec((row_count, model_width), lambda i: (0, 0)))
        scratch.append(pltpu.VMEM((row_count, model_width), jnp.float32))
    flops = 2 * (3 if with_grads else 2) * row_count * model_width * hidden_width
    moved = 2 * 2 * model_width * hidden_width
    return pl.pallas_call(
        hidden_kernel,
        grid=(hidden_width // tile,),
        out_shape=out_shape,
        in_specs=[
            pl.BlockSpec((row_count, width), lambda i: (0, 0)),
            pl.BlockSpec((model_width, tile), lambda i: (0, i)),
            pl.BlockSpec((tile, model_width), lambda i: (i, 0)),
        ],
        out_specs=out_specs,
        scratch_shapes=scratch,
        compiler_params=pltpu.CompilerParams(dimension_semantics=("arbitrary",)),
        cost_estimate=pl.CostEstimate(flops=flops, bytes_accessed=moved, transcendentals=0),
        name="hidden_parts",
    )(rows, first_weight, second_weight)


def weights_kernel(part_count, steps, half_ref, *refs):
    x_refs = refs[:part_count]
    cot_refs = refs[part_count : 2 * part_count]
    act_refs = refs[2 * part_count : 3 * part_count]
    pre_refs = refs[3 * part_count : 4 * part_count]
    first_ref, second_ref, x_scratch = refs[4 * part_count :]
    step = pl.program_id(0)

    @pl.when(step == 0)
    def _():
        place = 0
        for ref in x_refs:
            count = ref.shape[0]
            x_scratch[:, place : place + count] = ref[...].T
            place += count

    @pl.when(step < steps[0])
    def _():
        place = 0
        total = None
        for ref in pre_refs:
            count = ref.shape[0]
            part = contract(x_scratch[:, place : place + count], ref[...], 1, 0)
            total = part if total is None else total + part
            place += count
        first_ref[...] = total * grad_scale

    @pl.when(step >= steps[0])
    def _():
        total = None
        for act, cot in zip(act_refs, cot_refs):
            part = contract(act[...].T, cot[...], 1, 0)
            total = part if total is None else total + part
        second_ref[...] = total * grad_scale


def weight_grads(half_index, rows, acts, pres, halves, model_width, hidden_width):
    first_rows = model_width // halves
    second_rows = hidden_width // halves
    steps = (4, 4)
    first_tile = hidden_width // steps[0]
    second_tile = second_rows // steps[1]
    row_count = sum(part.shape[0] for part in rows)
    flops = 4 * row_count * first_rows * hidden_width

    def early(i):
        return jnp.minimum(i, steps[0] - 1)

    def late(i):
        return jnp.maximum(i - steps[0], 0)

    counts = [part.shape[0] for part in rows]
    in_specs = [pl.BlockSpec((n, first_rows), lambda i, h: (0, h[0])) for n in counts]
    in_specs += [pl.BlockSpec((n, model_width), lambda i, h: (0, 1)) for n in counts]
    in_specs += [
        pl.BlockSpec((n, second_tile), lambda i, h: (0, h[0] * steps[1] + late(i)))
        for n in counts
    ]
    in_specs += [pl.BlockSpec((n, first_tile), lambda i, h: (0, early(i))) for n in counts]
    return pl.pallas_call(
        functools.partial(weights_kernel, len(rows), steps),
        grid_spec=pltpu.PrefetchScalarGridSpec(
            num_scalar_prefetch=1,
            grid=(sum(steps),),
            in_specs=in_specs,
            out_specs=[
                pl.BlockSpec((first_rows, first_tile), lambda i, h: (0, early(i))),
                pl.BlockSpec((second_tile, model_width), lambda i, h: (late(i), 0)),
            ],
            scratch_shapes=[pltpu.VMEM((first_rows, row_count), jnp.bfloat16)],
        ),
        out_shape=[
            jax.ShapeDtypeStruct((first_rows, hidden_width), jnp.float32),
            jax.ShapeDtypeStruct((second_rows, model_width), jnp.float32),
        ],
        compiler_params=pltpu.CompilerParams(dimension_semantics=("arbitrary",)),
        cost_estimate=pl.CostEstimate(
            flops=flops, bytes_accessed=8 * first_rows * hidden_width, transcendentals=0
        ),
        name="weight_grads",
    )(jnp.reshape(half_index, (1,)), *rows, *rows, *acts, *pres)


def on_device(inputs, cotangent, task_ids, group_counts, task_gate, w_in, w_out):
    groups = group_counts.shape[1]
    model_width = inputs.shape[1]
    capacity = inputs.shape[0] // groups
    repeats = lax.axis_size("rep")
    halves = lax.axis_size("dp")
    own_repeat = lax.axis_index("rep")
    half_index = lax.axis_index("dp")
    first_weight = w_in[0]
    second_weight = w_out[0]
    hidden_width = first_weight.shape[1]
    outgoing, near = pack_blocks(
        (repeats, groups, halves, capacity), task_ids, group_counts, task_gate, inputs, cotangent
    )
    width = outgoing.shape[-1]

    def across(turn, step):
        pairs = []
        for source in range(groups * halves):
            group, half = divmod(source, halves)
            target = partner_of(group, step, groups) * halves + (half + turn) % halves
            pairs.append((source, target))
        return pairs

    own_rows = lax.all_to_all(outgoing, ("rep", "grp"), 0, 0)
    near_other = [
        lax.ppermute(near[step], ("grp", "dp"), across(turn, step))
        for turn in range(1, halves)
        for step in range(groups)
    ]
    own_three = own_rows.reshape(repeats, groups * capacity, width)
    far_other = []
    for hop in range(1, repeats):
        source = lax.rem(own_repeat + hop, repeats)
        far_rows = lax.dynamic_index_in_dim(own_three, source, 0, keepdims=False)
        for turn in range(1, halves):
            pairs = [(i, (i + turn) % halves) for i in range(halves)]
            far_other.append(lax.ppermute(far_rows, "dp", pairs))
    own = own_rows.reshape(repeats * groups * capacity, width)
    act, pre, row_grads = hidden_parts(own, first_weight, second_weight, True)
    rows, acts, pres = [own], [act], [pre]
    returned = lax.all_to_all(
        row_grads.reshape(repeats * groups, capacity, model_width), ("rep", "grp"), 0, 0
    )
    for pieces in (near_other, far_other):
        if pieces:
            part = pieces[0] if len(pieces) == 1 else jnp.concatenate(pieces)
            act, pre = hidden_parts(part, first_weight, second_weight, False)
            rows.append(part)
            acts.append(act)
            pres.append(pre)
    grad_first, grad_second = weight_grads(
        half_index, rows, acts, pres, halves, model_width, hidden_width
    )
    input_home = jnp.sum(
        returned.reshape(repeats, groups * capacity, model_width).astype(jnp.float32), axis=0
    )
    return (input_home, grad_first[None], grad_second[None])


def solution(mesh):
    def step(inputs, cotangent, task_ids, group_counts, task_gate, w_in, w_out):
        groups = group_counts.shape[1]
        halves = mesh.shape["dp"]
        repeats = mesh.shape["blk"] // groups
        fine = Mesh(mesh.devices.reshape(repeats, groups, halves), ("rep", "grp", "dp"))
        rows = P(("rep", "grp", "dp"))
        expert = P(("rep", "grp"))
        split = P(("rep", "grp"), "dp")
        return jax.shard_map(
            on_device,
            mesh=fine,
            in_specs=(rows, rows, rows, rows, P(), expert, expert),
            out_specs=(rows, split, split),
            check_vma=False,
        )(inputs, cotangent, task_ids, group_counts, task_gate, w_in, w_out)

    return step
```

```python
import functools

import jax
import jax.numpy as jnp
from jax import lax
from jax.experimental import pallas as pl
from jax.experimental.pallas import tpu as pltpu
from jax.sharding import Mesh
from jax.sharding import PartitionSpec as P


grad_scale = 0.0625
lanes = 128
own_tile = 256
rest_tile = 512
kernel_grant = 48 << 20


smem_spec = pl.BlockSpec(memory_space=pltpu.SMEM)
vmem_spec = pl.BlockSpec(memory_space=pltpu.VMEM)
hbm_spec = pl.BlockSpec(memory_space=pltpu.HBM)
any_spec = pl.BlockSpec(memory_space=pl.ANY)


def contract(left, right, left_dim, right_dim):
    return lax.dot_general(
        left, right, (((left_dim,), (right_dim,)), ((), ())), preferred_element_type=jnp.float32
    )


def partner_of(group, step, groups):
    if groups & (groups - 1) == 0:
        return group ^ step
    return (group + step) % groups


def partner(group, step, groups, sign):
    if groups & (groups - 1) == 0:
        return group ^ step
    return lax.rem(group + sign * step + groups, groups)


def pack_kernel(repeats, groups, capacity, ids, counts, table, x_ref, cot_ref, *outs):
    all_ref, near_refs = outs[0], outs[1:]
    model_width = x_ref.shape[1]
    task_count = table.shape[0]
    own_repeat = lax.axis_index("rep")
    own_group = lax.axis_index("grp")
    row = lax.broadcasted_iota(jnp.int32, (capacity, lanes), 0)
    for step in range(groups):
        group = partner(own_group, step, groups, 1)
        start = pl.multiple_of(group * capacity, capacity)
        live = counts[0, group]
        tags = jnp.full((capacity, lanes), task_count, jnp.int32)
        for slot in range(capacity):
            tags = jnp.where(row == slot, ids[start + slot], tags)
        tags = jnp.where(row < live, tags, task_count)
        rows = pl.ds(start, capacity)
        for hop in range(repeats):
            expert = lax.rem(own_repeat + hop, repeats) * groups + group
            block_refs = [all_ref.at[expert]]
            if hop == 0 and near_refs:
                block_refs.append(near_refs[step])
            gate = jnp.zeros((capacity, lanes), jnp.float32)
            for task in range(task_count):
                gate = jnp.where(tags == task, table[task, expert], gate)
            for ref in block_refs:
                ref[:, :model_width] = x_ref[rows, :]
            for column in range(0, model_width, lanes):
                part = cot_ref[rows, column : column + lanes].astype(jnp.float32) * gate
                part = part.astype(jnp.bfloat16)
                for ref in block_refs:
                    ref[:, model_width + column : model_width + column + lanes] = part


def pack_blocks(sizes, task_ids, group_counts, task_gate, inputs, cotangent):
    repeats, groups, halves, capacity = sizes
    width = 2 * inputs.shape[1]
    near_count = groups if halves > 1 else 0
    out_shape = [jax.ShapeDtypeStruct((repeats * groups, capacity, width), jnp.bfloat16)]
    out_shape += [jax.ShapeDtypeStruct((capacity, width), jnp.bfloat16)] * near_count
    outs = pl.pallas_call(
        functools.partial(pack_kernel, repeats, groups, capacity),
        out_shape=out_shape,
        in_specs=[smem_spec, smem_spec, smem_spec, vmem_spec, vmem_spec],
        out_specs=[vmem_spec] * len(out_shape),
        name="pack_blocks",
    )(task_ids, group_counts, task_gate, inputs, cotangent)
    return outs[0], outs[1:]


def weight_copies(tile, first_hbm, second_hbm, first_ref, second_ref, sems):
    copies = []
    for index in range(first_ref.shape[1] // tile):
        part = slice(index * tile, (index + 1) * tile)
        copies.append(
            (
                pltpu.make_async_copy(
                    first_hbm.at[:, part], first_ref.at[:, part], sems.at[2 * index]
                ),
                pltpu.make_async_copy(
                    second_hbm.at[part, :], second_ref.at[part, :], sems.at[2 * index + 1]
                ),
            )
        )
    for pair in copies:
        for copy in pair:
            copy.start()
    return copies


def wait_pair(pair):
    for copy in pair:
        copy.wait()


def weight_scratch(first_weight, second_weight, tile):
    return [
        pltpu.VMEM(first_weight.shape, first_weight.dtype),
        pltpu.VMEM(second_weight.shape, second_weight.dtype),
        pltpu.SemaphoreType.DMA((2 * first_weight.shape[1] // tile,)),
    ]


def hidden_chunk(x_rows, scaled_cot, first, second):
    pre_act = contract(x_rows, first, 1, 0)
    hidden_cot = contract(scaled_cot, second, 1, 1)
    sigmoid_act = 1.0 / (1.0 + jnp.exp(-pre_act))
    value = pre_act * sigmoid_act
    slope = sigmoid_act * (1.0 + pre_act - value)
    return value.astype(jnp.bfloat16), (hidden_cot * slope).astype(jnp.bfloat16)


def own_kernel(repeats, after_count, rows_ref, first_hbm, second_hbm, *refs):
    act_ref, pre_ref, grad_ref, far_ref, first_ref, second_ref, sems = refs[after_count:]
    row_count = rows_ref.shape[0]
    model_width, hidden_width = first_ref.shape
    copies = weight_copies(own_tile, first_hbm, second_hbm, first_ref, second_ref, sems)
    per_repeat = row_count // repeats
    own_repeat = lax.axis_index("rep")
    for hop in range(1, repeats):
        source = lax.rem(own_repeat + hop, repeats)
        start = pl.multiple_of(source * per_repeat, per_repeat)
        far_ref[hop - 1] = rows_ref[pl.ds(start, per_repeat), :]
    x_rows = rows_ref[:, :model_width]
    scaled_cot = rows_ref[:, model_width:]
    for index, start in enumerate(range(0, hidden_width, own_tile)):
        columns = slice(start, start + own_tile)
        wait_pair(copies[index])
        act, pre = hidden_chunk(x_rows, scaled_cot, first_ref[:, columns], second_ref[columns, :])
        act_ref[:, columns] = act
        pre_ref[:, columns] = pre
    grad_ref[...] = contract(pre_ref[...], first_ref[...], 1, 1).astype(jnp.bfloat16)


def own_parts(repeats, rows, first_weight, second_weight, after):
    row_count, width = rows.shape
    model_width, hidden_width = first_weight.shape
    wide = jax.ShapeDtypeStruct((row_count, hidden_width), jnp.bfloat16)
    return pl.pallas_call(
        functools.partial(own_kernel, repeats, len(after)),
        out_shape=[
            wide,
            wide,
            jax.ShapeDtypeStruct((row_count, model_width), jnp.bfloat16),
            jax.ShapeDtypeStruct((repeats - 1, row_count // repeats, width), jnp.bfloat16),
        ],
        in_specs=[vmem_spec, any_spec, any_spec] + [any_spec] * len(after),
        out_specs=[vmem_spec] * 4,
        scratch_shapes=weight_scratch(first_weight, second_weight, own_tile),
        compiler_params=pltpu.CompilerParams(vmem_limit_bytes=kernel_grant),
        cost_estimate=pl.CostEstimate(
            flops=6 * row_count * model_width * hidden_width,
            bytes_accessed=4 * model_width * hidden_width,
            transcendentals=0,
        ),
        name="own_parts",
    )(rows, first_weight, second_weight, *after)


def rest_kernel(other_count, own_ref, act_ref, pre_ref, *refs):
    other_refs = refs[:other_count]
    first_hbm, second_hbm, first_out, second_out = refs[other_count : other_count + 4]
    other, other_act, left, first_buf, second_buf, sems = refs[other_count + 4 : other_count + 10]
    first_ref, second_ref, weight_sems = refs[other_count + 10 :]
    loads = weight_copies(rest_tile, first_hbm, second_hbm, first_ref, second_ref, weight_sems)
    own_count = own_ref.shape[0]
    model_width, _ = first_ref.shape
    first_tiles, first_rows, first_tile = first_buf.shape
    second_tiles, second_tile, _ = second_buf.shape
    half = lax.axis_index("dp")
    place = 0
    for ref in other_refs:
        other[place : place + ref.shape[0], :] = ref[...]
        place += ref.shape[0]
    x_begin = pl.multiple_of(half * first_rows, first_rows)
    left[:, :own_count] = own_ref[:, pl.ds(x_begin, first_rows)].T
    left[:, own_count:] = other[:, pl.ds(x_begin, first_rows)].T
    copies = []
    for tile in range(first_tiles):
        columns = slice(tile * first_tile, (tile + 1) * first_tile)
        wait_pair(loads[tile])
        act, pre = hidden_chunk(
            other[:, :model_width],
            other[:, model_width:],
            first_ref[:, columns],
            second_ref[columns, :],
        )
        other_act[:, columns] = act
        total = contract(left[:, :own_count], pre_ref[:, columns], 1, 0)
        total += contract(left[:, own_count:], pre, 1, 0)
        first_buf[tile] = total * grad_scale
        if copies:
            copies[-1].start()
        copies.append(
            pltpu.make_async_copy(first_buf.at[tile], first_out.at[:, columns], sems.at[tile])
        )
    for tile in range(second_tiles):
        begin = half * (second_tiles * second_tile) + tile * second_tile
        columns = pl.ds(pl.multiple_of(begin, second_tile), second_tile)
        total = contract(act_ref[:, columns].T, own_ref[:, model_width:], 1, 0)
        total += contract(other_act[:, columns].T, other[:, model_width:], 1, 0)
        second_buf[tile] = total * grad_scale
        copies[-1].start()
        rows = slice(tile * second_tile, (tile + 1) * second_tile)
        copies.append(
            pltpu.make_async_copy(
                second_buf.at[tile], second_out.at[rows, :], sems.at[first_tiles + tile]
            )
        )
    copies[-1].start()
    for copy in copies:
        copy.wait()


def rest_parts(halves, own, act, pre, others, first_weight, second_weight):
    own_count, width = own.shape
    model_width, hidden_width = first_weight.shape
    other_rows = sum(part.shape[0] for part in others)
    first_rows, second_rows = model_width // halves, hidden_width // halves
    first_tiles = hidden_width // rest_tile
    second_tiles = second_rows // rest_tile
    row_count = own_count + other_rows
    flops = 4 * (row_count * first_rows + other_rows * model_width) * hidden_width
    return pl.pallas_call(
        functools.partial(rest_kernel, len(others)),
        out_shape=[
            jax.ShapeDtypeStruct((first_rows, hidden_width), jnp.float32),
            jax.ShapeDtypeStruct((second_rows, model_width), jnp.float32),
        ],
        in_specs=[vmem_spec] * (3 + len(others)) + [any_spec] * 2,
        out_specs=[hbm_spec, hbm_spec],
        scratch_shapes=[
            pltpu.VMEM((other_rows, width), jnp.bfloat16),
            pltpu.VMEM((other_rows, hidden_width), jnp.bfloat16),
            pltpu.VMEM((first_rows, row_count), jnp.bfloat16),
            pltpu.VMEM((first_tiles, first_rows, rest_tile), jnp.float32),
            pltpu.VMEM((second_tiles, rest_tile, model_width), jnp.float32),
            pltpu.SemaphoreType.DMA((first_tiles + second_tiles,)),
            *weight_scratch(first_weight, second_weight, rest_tile),
        ],
        compiler_params=pltpu.CompilerParams(vmem_limit_bytes=kernel_grant),
        cost_estimate=pl.CostEstimate(
            flops=flops, bytes_accessed=8 * first_rows * hidden_width, transcendentals=0
        ),
        name="rest_parts",
    )(own, act, pre, *others, first_weight, second_weight)


def on_device(inputs, cotangent, task_ids, group_counts, task_gate, w_in, w_out):
    groups = group_counts.shape[1]
    model_width = inputs.shape[1]
    capacity = inputs.shape[0] // groups
    repeats = lax.axis_size("rep")
    halves = lax.axis_size("dp")
    first_weight = w_in[0]
    second_weight = w_out[0]
    outgoing, near = pack_blocks(
        (repeats, groups, halves, capacity), task_ids, group_counts, task_gate, inputs, cotangent
    )
    width = outgoing.shape[-1]

    def across(turn, step):
        pairs = []
        for source in range(groups * halves):
            group, half = divmod(source, halves)
            target = partner_of(group, step, groups) * halves + (half + turn) % halves
            pairs.append((source, target))
        return pairs

    own_rows = lax.all_to_all(outgoing, ("rep", "grp"), 0, 0)
    near_other = [
        lax.ppermute(near[step], ("grp", "dp"), across(turn, step))
        for turn in range(1, halves)
        for step in range(groups)
    ]
    own = own_rows.reshape(repeats * groups * capacity, width)
    act, pre, row_grads, far_rows = own_parts(repeats, own, first_weight, second_weight, [])
    far_other = []
    for hop in range(repeats - 1):
        for turn in range(1, halves):
            pairs = [(i, (i + turn) % halves) for i in range(halves)]
            far_other.append(lax.ppermute(far_rows[hop], "dp", pairs))
    returned = lax.all_to_all(
        row_grads.reshape(repeats * groups, capacity, model_width), ("rep", "grp"), 0, 0
    )
    grad_first, grad_second = rest_parts(
        halves, own, act, pre, near_other + far_other, first_weight, second_weight
    )
    input_home = jnp.sum(
        returned.reshape(repeats, groups * capacity, model_width).astype(jnp.float32), axis=0
    )
    return (input_home, grad_first[None], grad_second[None])


def solution(mesh):

    def step(inputs, cotangent, task_ids, group_counts, task_gate, w_in, w_out):
        groups = group_counts.shape[1]
        halves = mesh.shape["dp"]
        repeats = mesh.shape["blk"] // groups
        fine = Mesh(mesh.devices.reshape(repeats, groups, halves), ("rep", "grp", "dp"))
        rows = P(("rep", "grp", "dp"))
        expert = P(("rep", "grp"))
        split = P(("rep", "grp"), "dp")
        return jax.shard_map(
            on_device,
            mesh=fine,
            in_specs=(rows, rows, rows, rows, P(), expert, expert),
            out_specs=(rows, split, split),
            check_vma=False,
        )(inputs, cotangent, task_ids, group_counts, task_gate, w_in, w_out)

    return step
```

```python
import functools

import jax
import jax.numpy as jnp
from jax import lax
from jax.experimental import pallas as pl
from jax.experimental.pallas import tpu as pltpu
from jax.sharding import Mesh
from jax.sharding import PartitionSpec as P


grad_scale = 0.0625
lanes = 128
own_tile = 256
rest_tile = 512
kernel_grant = 48 << 20
load_depth = 4
stage_grant = 1 << 20


smem_spec = pl.BlockSpec(memory_space=pltpu.SMEM)
vmem_spec = pl.BlockSpec(memory_space=pltpu.VMEM)
hbm_spec = pl.BlockSpec(memory_space=pltpu.HBM)
any_spec = pl.BlockSpec(memory_space=pl.ANY)


def contract(left, right, left_dim, right_dim):
    return lax.dot_general(
        left, right, (((left_dim,), (right_dim,)), ((), ())), preferred_element_type=jnp.float32
    )


def partner_of(group, step, groups):
    if groups & (groups - 1) == 0:
        return group ^ step
    return (group + step) % groups


def partner(group, step, groups, sign):
    if groups & (groups - 1) == 0:
        return group ^ step
    return lax.rem(group + sign * step + groups, groups)


def pack_kernel(repeats, groups, capacity, ids, counts, table, x_ref, cot_ref, *outs):
    all_ref, near_refs = outs[0], outs[1:]
    model_width = x_ref.shape[1]
    task_count = table.shape[0]
    own_repeat = lax.axis_index("rep")
    own_group = lax.axis_index("grp")
    row = lax.broadcasted_iota(jnp.int32, (capacity, lanes), 0)
    for step in range(groups):
        group = partner(own_group, step, groups, 1)
        start = pl.multiple_of(group * capacity, capacity)
        live = counts[0, group]
        tags = jnp.full((capacity, lanes), task_count, jnp.int32)
        for slot in range(capacity):
            tags = jnp.where(row == slot, ids[start + slot], tags)
        tags = jnp.where(row < live, tags, task_count)
        rows = pl.ds(start, capacity)
        for hop in range(repeats):
            expert = lax.rem(own_repeat + hop, repeats) * groups + group
            block_refs = [all_ref.at[expert]]
            if hop == 0 and near_refs:
                block_refs.append(near_refs[step])
            gate = jnp.zeros((capacity, lanes), jnp.float32)
            for task in range(task_count):
                gate = jnp.where(tags == task, table[task, expert], gate)
            for ref in block_refs:
                ref[:, :model_width] = x_ref[rows, :]
            for column in range(0, model_width, lanes):
                part = cot_ref[rows, column : column + lanes].astype(jnp.float32) * gate
                part = part.astype(jnp.bfloat16)
                for ref in block_refs:
                    ref[:, model_width + column : model_width + column + lanes] = part


def pack_blocks(sizes, task_ids, group_counts, task_gate, inputs, cotangent):
    repeats, groups, halves, capacity = sizes
    width = 2 * inputs.shape[1]
    near_count = groups if halves > 1 else 0
    out_shape = [jax.ShapeDtypeStruct((repeats * groups, capacity, width), jnp.bfloat16)]
    out_shape += [jax.ShapeDtypeStruct((capacity, width), jnp.bfloat16)] * near_count
    outs = pl.pallas_call(
        functools.partial(pack_kernel, repeats, groups, capacity),
        out_shape=out_shape,
        in_specs=[smem_spec, smem_spec, smem_spec, vmem_spec, vmem_spec],
        out_specs=[vmem_spec] * len(out_shape),
        name="pack_blocks",
    )(task_ids, group_counts, task_gate, inputs, cotangent)
    return outs[0], outs[1:]


def weight_copies(tile, first_hbm, second_hbm, first_ref, second_ref, sems):
    copies = []
    for index in range(first_ref.shape[1] // tile):
        part = slice(index * tile, (index + 1) * tile)
        copies.append(
            (
                pltpu.make_async_copy(
                    first_hbm.at[:, part], first_ref.at[:, part], sems.at[2 * index]
                ),
                pltpu.make_async_copy(
                    second_hbm.at[part, :], second_ref.at[part, :], sems.at[2 * index + 1]
                ),
            )
        )
    for pair in copies[:load_depth]:
        start_pair(pair)
    return copies


def start_pair(pair):
    for copy in pair:
        copy.start()


def wait_pair(pair):
    for copy in pair:
        copy.wait()


def next_pair(copies, index):
    if index + load_depth < len(copies):
        start_pair(copies[index + load_depth])
    wait_pair(copies[index])


def weight_scratch(first_weight, second_weight, tile):
    return [
        pltpu.VMEM(first_weight.shape, first_weight.dtype),
        pltpu.VMEM(second_weight.shape, second_weight.dtype),
        pltpu.SemaphoreType.DMA((2 * first_weight.shape[1] // tile,)),
    ]


def hidden_chunk(x_rows, scaled_cot, first, second):
    pre_act = contract(x_rows, first, 1, 0)
    hidden_cot = contract(scaled_cot, second, 1, 1)
    sigmoid_act = 1.0 / (1.0 + jnp.exp(-pre_act))
    value = pre_act * sigmoid_act
    slope = sigmoid_act * (1.0 + pre_act - value)
    return value.astype(jnp.bfloat16), (hidden_cot * slope).astype(jnp.bfloat16)


def own_kernel(repeats, rows_ref, first_hbm, second_hbm, *refs):
    act_hbm, pre_hbm, grad_ref, far_ref = refs[:4]
    act_ref, pre_ref, total_ref, out_sems, first_ref, second_ref, sems = refs[4:]
    row_count = rows_ref.shape[0]
    model_width, hidden_width = first_ref.shape
    copies = weight_copies(own_tile, first_hbm, second_hbm, first_ref, second_ref, sems)
    per_repeat = row_count // repeats
    own_repeat = lax.axis_index("rep")
    for hop in range(1, repeats):
        source = lax.rem(own_repeat + hop, repeats)
        start = pl.multiple_of(source * per_repeat, per_repeat)
        far_ref[hop - 1] = rows_ref[pl.ds(start, per_repeat), :]
    x_rows = rows_ref[:, :model_width]
    scaled_cot = rows_ref[:, model_width:]
    stores = []
    last = hidden_width // own_tile - 1
    for index in range(last + 1):
        columns = slice(index * own_tile, (index + 1) * own_tile)
        next_pair(copies, index)
        act, pre = hidden_chunk(x_rows, scaled_cot, first_ref[:, columns], second_ref[columns, :])
        act_ref[:, columns] = act
        pre_ref[:, columns] = pre
        part = contract(pre, first_ref[:, columns], 1, 1)
        if index == 0:
            total_ref[...] = part
        elif index < last:
            total_ref[...] += part
        else:
            grad_ref[...] = (total_ref[...] + part).astype(jnp.bfloat16)
        stores.append(
            (
                pltpu.make_async_copy(
                    act_ref.at[:, columns], act_hbm.at[:, columns], out_sems.at[2 * index]
                ),
                pltpu.make_async_copy(
                    pre_ref.at[:, columns], pre_hbm.at[:, columns], out_sems.at[2 * index + 1]
                ),
            )
        )
        start_pair(stores[-1])
    for pair in stores:
        wait_pair(pair)


def own_parts(repeats, rows, first_weight, second_weight):
    row_count, width = rows.shape
    model_width, hidden_width = first_weight.shape
    wide = jax.ShapeDtypeStruct((row_count, hidden_width), jnp.bfloat16)
    return pl.pallas_call(
        functools.partial(own_kernel, repeats),
        out_shape=[
            wide,
            wide,
            jax.ShapeDtypeStruct((row_count, model_width), jnp.bfloat16),
            jax.ShapeDtypeStruct((repeats - 1, row_count // repeats, width), jnp.bfloat16),
        ],
        in_specs=[vmem_spec, any_spec, any_spec],
        out_specs=[hbm_spec, hbm_spec, vmem_spec, vmem_spec],
        scratch_shapes=[
            pltpu.VMEM(wide.shape, wide.dtype),
            pltpu.VMEM(wide.shape, wide.dtype),
            pltpu.VMEM((row_count, model_width), jnp.float32),
            pltpu.SemaphoreType.DMA((2 * hidden_width // own_tile,)),
            *weight_scratch(first_weight, second_weight, own_tile),
        ],
        compiler_params=pltpu.CompilerParams(vmem_limit_bytes=kernel_grant),
        cost_estimate=pl.CostEstimate(
            flops=6 * row_count * model_width * hidden_width,
            bytes_accessed=4 * model_width * hidden_width,
            transcendentals=0,
        ),
        name="own_parts",
    )(rows, first_weight, second_weight)


def stage_kernel(count, *refs):
    sems = refs[-1]
    copies = [
        pltpu.make_async_copy(refs[i], refs[count + i], sems.at[i]) for i in range(count)
    ]
    start_pair(copies)
    wait_pair(copies)


def stage(arrays):
    count = len(arrays)
    return pl.pallas_call(
        functools.partial(stage_kernel, count),
        out_shape=[jax.ShapeDtypeStruct(part.shape, part.dtype) for part in arrays],
        in_specs=[any_spec] * count,
        out_specs=[any_spec] * count,
        scratch_shapes=[pltpu.SemaphoreType.DMA((count,))],
        compiler_params=pltpu.CompilerParams(vmem_limit_bytes=stage_grant),
        name="stage",
    )(*arrays)


def rest_kernel(other_count, own_ref, act_ref, pre_ref, *refs):
    other_refs = refs[:other_count]
    first_ref, second_ref, first_out, second_out = refs[other_count : other_count + 4]
    other, other_act, left, first_buf, second_buf, sems = refs[other_count + 4 :]
    own_count = own_ref.shape[0]
    model_width, _ = first_ref.shape
    first_tiles, first_rows, first_tile = first_buf.shape
    second_tiles, second_tile, _ = second_buf.shape
    half = lax.axis_index("dp")
    place = 0
    for ref in other_refs:
        other[place : place + ref.shape[0], :] = ref[...]
        place += ref.shape[0]
    x_begin = pl.multiple_of(half * first_rows, first_rows)
    left[:, :own_count] = own_ref[:, pl.ds(x_begin, first_rows)].T
    left[:, own_count:] = other[:, pl.ds(x_begin, first_rows)].T
    copies = []
    for tile in range(first_tiles):
        columns = slice(tile * first_tile, (tile + 1) * first_tile)
        act, pre = hidden_chunk(
            other[:, :model_width],
            other[:, model_width:],
            first_ref[:, columns],
            second_ref[columns, :],
        )
        other_act[:, columns] = act
        total = contract(left[:, :own_count], pre_ref[:, columns], 1, 0)
        total += contract(left[:, own_count:], pre, 1, 0)
        first_buf[tile] = total * grad_scale
        if copies:
            copies[-1].start()
        copies.append(
            pltpu.make_async_copy(first_buf.at[tile], first_out.at[:, columns], sems.at[tile])
        )
    for tile in range(second_tiles):
        begin = half * (second_tiles * second_tile) + tile * second_tile
        columns = pl.ds(pl.multiple_of(begin, second_tile), second_tile)
        total = contract(act_ref[:, columns].T, own_ref[:, model_width:], 1, 0)
        total += contract(other_act[:, columns].T, other[:, model_width:], 1, 0)
        second_buf[tile] = total * grad_scale
        copies[-1].start()
        rows = slice(tile * second_tile, (tile + 1) * second_tile)
        copies.append(
            pltpu.make_async_copy(
                second_buf.at[tile], second_out.at[rows, :], sems.at[first_tiles + tile]
            )
        )
    copies[-1].start()
    for copy in copies:
        copy.wait()


def rest_parts(halves, own, act, pre, others, first_weight, second_weight):
    own_count, width = own.shape
    model_width, hidden_width = first_weight.shape
    other_rows = sum(part.shape[0] for part in others)
    first_rows, second_rows = model_width // halves, hidden_width // halves
    first_tiles = hidden_width // rest_tile
    second_tiles = second_rows // rest_tile
    row_count = own_count + other_rows
    flops = 4 * (row_count * first_rows + other_rows * model_width) * hidden_width
    return pl.pallas_call(
        functools.partial(rest_kernel, len(others)),
        out_shape=[
            jax.ShapeDtypeStruct((first_rows, hidden_width), jnp.float32),
            jax.ShapeDtypeStruct((second_rows, model_width), jnp.float32),
        ],
        in_specs=[vmem_spec] * (5 + len(others)),
        out_specs=[hbm_spec, hbm_spec],
        scratch_shapes=[
            pltpu.VMEM((other_rows, width), jnp.bfloat16),
            pltpu.VMEM((other_rows, hidden_width), jnp.bfloat16),
            pltpu.VMEM((first_rows, row_count), jnp.bfloat16),
            pltpu.VMEM((first_tiles, first_rows, rest_tile), jnp.float32),
            pltpu.VMEM((second_tiles, rest_tile, model_width), jnp.float32),
            pltpu.SemaphoreType.DMA((first_tiles + second_tiles,)),
        ],
        compiler_params=pltpu.CompilerParams(
            vmem_limit_bytes=min(60 << 20, (16 << 20) + row_count * (32 << 10))
        ),
        cost_estimate=pl.CostEstimate(
            flops=flops, bytes_accessed=8 * first_rows * hidden_width, transcendentals=0
        ),
        name="rest_parts",
    )(own, act, pre, *others, first_weight, second_weight)


def on_device(inputs, cotangent, task_ids, group_counts, task_gate, w_in, w_out):
    groups = group_counts.shape[1]
    model_width = inputs.shape[1]
    capacity = inputs.shape[0] // groups
    repeats = lax.axis_size("rep")
    halves = lax.axis_size("dp")
    first_weight = w_in[0]
    second_weight = w_out[0]
    outgoing, near = pack_blocks(
        (repeats, groups, halves, capacity), task_ids, group_counts, task_gate, inputs, cotangent
    )
    width = outgoing.shape[-1]

    def across(turn, step):
        pairs = []
        for source in range(groups * halves):
            group, half = divmod(source, halves)
            target = partner_of(group, step, groups) * halves + (half + turn) % halves
            pairs.append((source, target))
        return pairs

    own_rows = lax.all_to_all(outgoing, ("rep", "grp"), 0, 0)
    near_other = [
        lax.ppermute(near[step], ("grp", "dp"), across(turn, step))
        for turn in range(1, halves)
        for step in range(groups)
    ]
    own = own_rows.reshape(repeats * groups * capacity, width)
    act, pre, row_grads, far_rows = own_parts(repeats, own, first_weight, second_weight)
    far_other = []
    for hop in range(repeats - 1):
        for turn in range(1, halves):
            pairs = [(i, (i + turn) % halves) for i in range(halves)]
            far_other.append(lax.ppermute(far_rows[hop], "dp", pairs))
    returned = lax.all_to_all(
        row_grads.reshape(repeats * groups, capacity, model_width), ("rep", "grp"), 0, 0
    )
    own, act, pre, first_weight, second_weight = stage([own, act, pre, first_weight, second_weight])
    grad_first, grad_second = rest_parts(
        halves, own, act, pre, near_other + far_other, first_weight, second_weight
    )
    input_home = jnp.sum(
        returned.reshape(repeats, groups * capacity, model_width).astype(jnp.float32), axis=0
    )
    return (input_home, grad_first[None], grad_second[None])


def solution(mesh):

    def step(inputs, cotangent, task_ids, group_counts, task_gate, w_in, w_out):
        groups = group_counts.shape[1]
        halves = mesh.shape["dp"]
        repeats = mesh.shape["blk"] // groups
        fine = Mesh(mesh.devices.reshape(repeats, groups, halves), ("rep", "grp", "dp"))
        rows = P(("rep", "grp", "dp"))
        expert = P(("rep", "grp"))
        split = P(("rep", "grp"), "dp")
        return jax.shard_map(
            on_device,
            mesh=fine,
            in_specs=(rows, rows, rows, rows, P(), expert, expert),
            out_specs=(rows, split, split),
            check_vma=False,
        )(inputs, cotangent, task_ids, group_counts, task_gate, w_in, w_out)

    return step
```

```python
import functools

import jax
import jax.numpy as jnp
from jax import lax
from jax.experimental import pallas as pl
from jax.experimental.pallas import tpu as pltpu
from jax.sharding import Mesh
from jax.sharding import PartitionSpec as P


grad_scale = 0.0625
lanes = 128
own_tile = 512
rest_tile = 1024
last_tile = 512
kernel_grant = 48 << 20
load_depth = 4
stage_grant = 1 << 20


smem_spec = pl.BlockSpec(memory_space=pltpu.SMEM)
vmem_spec = pl.BlockSpec(memory_space=pltpu.VMEM)
hbm_spec = pl.BlockSpec(memory_space=pltpu.HBM)
any_spec = pl.BlockSpec(memory_space=pl.ANY)


def contract(left, right, left_dim, right_dim):
    return lax.dot_general(
        left, right, (((left_dim,), (right_dim,)), ((), ())), preferred_element_type=jnp.float32
    )


def partner_of(group, step, groups):
    if groups & (groups - 1) == 0:
        return group ^ step
    return (group + step) % groups


def partner(group, step, groups, sign):
    if groups & (groups - 1) == 0:
        return group ^ step
    return lax.rem(group + sign * step + groups, groups)


def pack_kernel(repeats, groups, capacity, ids, counts, table, x_ref, cot_ref, *outs):
    all_ref, near_refs = outs[0], outs[1:]
    model_width = x_ref.shape[1]
    task_count = table.shape[0]
    own_repeat = lax.axis_index("rep")
    own_group = lax.axis_index("grp")
    row = lax.broadcasted_iota(jnp.int32, (capacity, lanes), 0)
    for step in range(groups):
        group = partner(own_group, step, groups, 1)
        start = pl.multiple_of(group * capacity, capacity)
        live = counts[0, group]
        tags = jnp.full((capacity, lanes), task_count, jnp.int32)
        for slot in range(capacity):
            tags = jnp.where(row == slot, ids[start + slot], tags)
        tags = jnp.where(row < live, tags, task_count)
        rows = pl.ds(start, capacity)
        for hop in range(repeats):
            expert = lax.rem(own_repeat + hop, repeats) * groups + group
            block_refs = [all_ref.at[expert]]
            if hop == 0 and near_refs:
                block_refs.append(near_refs[step])
            gate = jnp.zeros((capacity, lanes), jnp.float32)
            for task in range(task_count):
                gate = jnp.where(tags == task, table[task, expert], gate)
            for ref in block_refs:
                ref[:, :model_width] = x_ref[rows, :]
            for column in range(0, model_width, lanes):
                part = cot_ref[rows, column : column + lanes].astype(jnp.float32) * gate
                part = part.astype(jnp.bfloat16)
                for ref in block_refs:
                    ref[:, model_width + column : model_width + column + lanes] = part


def pack_blocks(sizes, task_ids, group_counts, task_gate, inputs, cotangent):
    repeats, groups, halves, capacity = sizes
    width = 2 * inputs.shape[1]
    near_count = groups if halves > 1 else 0
    out_shape = [jax.ShapeDtypeStruct((repeats * groups, capacity, width), jnp.bfloat16)]
    out_shape += [jax.ShapeDtypeStruct((capacity, width), jnp.bfloat16)] * near_count
    outs = pl.pallas_call(
        functools.partial(pack_kernel, repeats, groups, capacity),
        out_shape=out_shape,
        in_specs=[smem_spec, smem_spec, smem_spec, vmem_spec, vmem_spec],
        out_specs=[vmem_spec] * len(out_shape),
        name="pack_blocks",
    )(task_ids, group_counts, task_gate, inputs, cotangent)
    return outs[0], outs[1:]


def weight_copies(tile, first_hbm, second_hbm, first_ref, second_ref, sems):
    copies = []
    for index in range(first_ref.shape[1] // tile):
        part = slice(index * tile, (index + 1) * tile)
        copies.append(
            (
                pltpu.make_async_copy(
                    first_hbm.at[:, part], first_ref.at[:, part], sems.at[2 * index]
                ),
                pltpu.make_async_copy(
                    second_hbm.at[part, :], second_ref.at[part, :], sems.at[2 * index + 1]
                ),
            )
        )
    for pair in copies[:load_depth]:
        start_pair(pair)
    return copies


def start_pair(pair):
    for copy in pair:
        copy.start()


def wait_pair(pair):
    for copy in pair:
        copy.wait()


def next_pair(copies, index):
    if index + load_depth < len(copies):
        start_pair(copies[index + load_depth])
    wait_pair(copies[index])


def weight_scratch(first_weight, second_weight, tile):
    return [
        pltpu.VMEM(first_weight.shape, first_weight.dtype),
        pltpu.VMEM(second_weight.shape, second_weight.dtype),
        pltpu.SemaphoreType.DMA((2 * first_weight.shape[1] // tile,)),
    ]


def hidden_chunk(x_rows, scaled_cot, first, second):
    pre_act = contract(x_rows, first, 1, 0)
    hidden_cot = contract(scaled_cot, second, 1, 1)
    sigmoid_act = 1.0 / (1.0 + jnp.exp(-pre_act))
    value = pre_act * sigmoid_act
    slope = sigmoid_act * (1.0 + pre_act - value)
    return value.astype(jnp.bfloat16), (hidden_cot * slope).astype(jnp.bfloat16)


def own_kernel(repeats, halves, rows_ref, first_hbm, second_hbm, *refs):
    act_out, pre_ref, x_ref, scaled_ref, grad_ref, far_ref = refs[:6]
    act_ref, total_ref, first_ref, second_ref, sems = refs[6:]
    row_count = rows_ref.shape[0]
    model_width, hidden_width = first_ref.shape
    copies = weight_copies(own_tile, first_hbm, second_hbm, first_ref, second_ref, sems)
    per_repeat = row_count // repeats
    own_repeat = lax.axis_index("rep")
    half = lax.axis_index("dp")
    for hop in range(1, repeats):
        source = lax.rem(own_repeat + hop, repeats)
        start = pl.multiple_of(source * per_repeat, per_repeat)
        far_ref[hop - 1] = rows_ref[pl.ds(start, per_repeat), :]
    first_rows = model_width // halves
    x_ref[...] = rows_ref[:, pl.ds(pl.multiple_of(half * first_rows, first_rows), first_rows)]
    scaled_ref[...] = rows_ref[:, model_width:]
    x_rows = rows_ref[:, :model_width]
    scaled_cot = rows_ref[:, model_width:]
    last = hidden_width // own_tile - 1
    for index in range(last + 1):
        columns = slice(index * own_tile, (index + 1) * own_tile)
        next_pair(copies, index)
        act, pre = hidden_chunk(x_rows, scaled_cot, first_ref[:, columns], second_ref[columns, :])
        act_ref[:, columns] = act
        pre_ref[:, columns] = pre
        if index == last:
            second_rows = hidden_width // halves
            begin = pl.multiple_of(half * second_rows, second_rows)
            act_out[...] = act_ref[:, pl.ds(begin, second_rows)]
        part = contract(pre, first_ref[:, columns], 1, 1)
        if index == 0:
            total_ref[...] = part
        elif index < last:
            total_ref[...] += part
        else:
            grad_ref[...] = (total_ref[...] + part).astype(jnp.bfloat16)


def own_parts(repeats, halves, rows, first_weight, second_weight):
    row_count, width = rows.shape
    model_width, hidden_width = first_weight.shape

    def shaped(*shape):
        return jax.ShapeDtypeStruct(shape, jnp.bfloat16)

    return pl.pallas_call(
        functools.partial(own_kernel, repeats, halves),
        out_shape=[
            shaped(row_count, hidden_width // halves),
            shaped(row_count, hidden_width),
            shaped(row_count, model_width // halves),
            shaped(row_count, model_width),
            shaped(row_count, model_width),
            shaped(repeats - 1, row_count // repeats, width),
        ],
        in_specs=[vmem_spec, any_spec, any_spec],
        out_specs=[vmem_spec] * 6,
        scratch_shapes=[
            pltpu.VMEM((row_count, hidden_width), jnp.bfloat16),
            pltpu.VMEM((row_count, model_width), jnp.float32),
            *weight_scratch(first_weight, second_weight, own_tile),
        ],
        compiler_params=pltpu.CompilerParams(vmem_limit_bytes=kernel_grant),
        cost_estimate=pl.CostEstimate(
            flops=6 * row_count * model_width * hidden_width,
            bytes_accessed=4 * model_width * hidden_width,
            transcendentals=0,
        ),
        name="own_parts",
    )(rows, first_weight, second_weight)


def stage_kernel(count, *refs):
    sems = refs[-1]
    copies = [
        pltpu.make_async_copy(refs[i], refs[count + i], sems.at[i]) for i in range(count)
    ]
    start_pair(copies)
    wait_pair(copies)


def stage(arrays):
    count = len(arrays)
    return pl.pallas_call(
        functools.partial(stage_kernel, count),
        out_shape=[jax.ShapeDtypeStruct(part.shape, part.dtype) for part in arrays],
        in_specs=[any_spec] * count,
        out_specs=[any_spec] * count,
        scratch_shapes=[pltpu.SemaphoreType.DMA((count,))],
        compiler_params=pltpu.CompilerParams(vmem_limit_bytes=stage_grant),
        name="stage",
    )(*arrays)


def rest_kernel(other_count, act_ref, pre_ref, x_ref, scaled_ref, *refs):
    other_refs = refs[:other_count]
    first_ref, second_ref, first_out, second_out = refs[other_count : other_count + 4]
    scratch = refs[other_count + 4 :]
    other, other_act, all_act, all_pre, scaled, left, first_buf, second_buf, sems = scratch
    own_count = act_ref.shape[0]
    model_width, _ = first_ref.shape
    first_tiles, first_rows, first_tile = first_buf.shape
    second_tiles, second_tile, _ = second_buf.shape
    half = lax.axis_index("dp")
    place = 0
    for ref in other_refs:
        other[place : place + ref.shape[0], :] = ref[...]
        place += ref.shape[0]
    x_begin = pl.multiple_of(half * first_rows, first_rows)
    left[:, :own_count] = x_ref[...].T
    left[:, own_count:] = other[:, pl.ds(x_begin, first_rows)].T
    scaled[:own_count, :] = scaled_ref[...]
    scaled[own_count:, :] = other[:, model_width:]
    all_act[:own_count, :] = act_ref[...]
    copies = []
    for tile in range(first_tiles):
        columns = slice(tile * first_tile, (tile + 1) * first_tile)
        act, pre = hidden_chunk(
            other[:, :model_width],
            other[:, model_width:],
            first_ref[:, columns],
            second_ref[columns, :],
        )
        other_act[:, columns] = act
        all_pre[:own_count, :] = pre_ref[:, columns]
        all_pre[own_count:, :] = pre
        first_buf[tile] = contract(left[...], all_pre[...], 1, 0) * grad_scale
        if copies:
            copies[-1].start()
        copies.append(
            pltpu.make_async_copy(first_buf.at[tile], first_out.at[:, columns], sems.at[tile])
        )
    second_rows = second_tiles * second_tile
    begin = pl.multiple_of(half * second_rows, second_rows)
    all_act[own_count:, :] = other_act[:, pl.ds(begin, second_rows)]
    for tile in range(second_tiles):
        rows = slice(tile * second_tile, (tile + 1) * second_tile)
        second_buf[tile] = contract(all_act[:, rows].T, scaled[...], 1, 0) * grad_scale
        copies[-1].start()
        copies.append(
            pltpu.make_async_copy(
                second_buf.at[tile], second_out.at[rows, :], sems.at[first_tiles + tile]
            )
        )
    copies[-1].start()
    for copy in copies:
        copy.wait()


def rest_parts(own, others, first_weight, second_weight):
    own_count, second_rows = own[0].shape
    first_rows = own[2].shape[1]
    width = others[0].shape[1]
    model_width, hidden_width = first_weight.shape
    other_rows = sum(part.shape[0] for part in others)
    first_tiles = hidden_width // rest_tile
    second_tiles = second_rows // last_tile
    row_count = own_count + other_rows
    flops = 4 * (row_count * first_rows + other_rows * model_width) * hidden_width
    return pl.pallas_call(
        functools.partial(rest_kernel, len(others)),
        out_shape=[
            jax.ShapeDtypeStruct((first_rows, hidden_width), jnp.float32),
            jax.ShapeDtypeStruct((second_rows, model_width), jnp.float32),
        ],
        in_specs=[vmem_spec] * (6 + len(others)),
        out_specs=[hbm_spec, hbm_spec],
        scratch_shapes=[
            pltpu.VMEM((other_rows, width), jnp.bfloat16),
            pltpu.VMEM((other_rows, hidden_width), jnp.bfloat16),
            pltpu.VMEM((row_count, second_rows), jnp.bfloat16),
            pltpu.VMEM((row_count, rest_tile), jnp.bfloat16),
            pltpu.VMEM((row_count, model_width), jnp.bfloat16),
            pltpu.VMEM((first_rows, row_count), jnp.bfloat16),
            pltpu.VMEM((first_tiles, first_rows, rest_tile), jnp.float32),
            pltpu.VMEM((second_tiles, last_tile, model_width), jnp.float32),
            pltpu.SemaphoreType.DMA((first_tiles + second_tiles,)),
        ],
        compiler_params=pltpu.CompilerParams(
            vmem_limit_bytes=min(60 << 20, (20 << 20) + row_count * (24 << 10))
        ),
        cost_estimate=pl.CostEstimate(
            flops=flops, bytes_accessed=8 * first_rows * hidden_width, transcendentals=0
        ),
        name="rest_parts",
    )(*own, *others, first_weight, second_weight)


def on_device(inputs, cotangent, task_ids, group_counts, task_gate, w_in, w_out):
    groups = group_counts.shape[1]
    model_width = inputs.shape[1]
    capacity = inputs.shape[0] // groups
    repeats = lax.axis_size("rep")
    halves = lax.axis_size("dp")
    first_weight = w_in[0]
    second_weight = w_out[0]
    outgoing, near = pack_blocks(
        (repeats, groups, halves, capacity), task_ids, group_counts, task_gate, inputs, cotangent
    )
    width = outgoing.shape[-1]

    def across(turn, step):
        pairs = []
        for source in range(groups * halves):
            group, half = divmod(source, halves)
            target = partner_of(group, step, groups) * halves + (half + turn) % halves
            pairs.append((source, target))
        return pairs

    own_rows = lax.all_to_all(outgoing, ("rep", "grp"), 0, 0)
    near_other = [
        lax.ppermute(near[step], ("grp", "dp"), across(turn, step))
        for turn in range(1, halves)
        for step in range(groups)
    ]
    own = own_rows.reshape(repeats * groups * capacity, width)
    *own_kept, row_grads, far_rows = own_parts(repeats, halves, own, first_weight, second_weight)
    far_other = []
    for hop in range(repeats - 1):
        for turn in range(1, halves):
            pairs = [(i, (i + turn) % halves) for i in range(halves)]
            far_other.append(lax.ppermute(far_rows[hop], "dp", pairs))
    returned = lax.all_to_all(
        row_grads.reshape(repeats * groups, capacity, model_width), ("rep", "grp"), 0, 0
    )
    *own_kept, first_weight, second_weight = stage([*own_kept, first_weight, second_weight])
    grad_first, grad_second = rest_parts(
        own_kept, near_other + far_other, first_weight, second_weight
    )
    input_home = jnp.sum(
        returned.reshape(repeats, groups * capacity, model_width).astype(jnp.float32), axis=0
    )
    return (input_home, grad_first[None], grad_second[None])


def solution(mesh):

    def step(inputs, cotangent, task_ids, group_counts, task_gate, w_in, w_out):
        groups = group_counts.shape[1]
        halves = mesh.shape["dp"]
        repeats = mesh.shape["blk"] // groups
        fine = Mesh(mesh.devices.reshape(repeats, groups, halves), ("rep", "grp", "dp"))
        rows = P(("rep", "grp", "dp"))
        expert = P(("rep", "grp"))
        split = P(("rep", "grp"), "dp")
        return jax.shard_map(
            on_device,
            mesh=fine,
            in_specs=(rows, rows, rows, rows, P(), expert, expert),
            out_specs=(rows, split, split),
            check_vma=False,
        )(inputs, cotangent, task_ids, group_counts, task_gate, w_in, w_out)

    return step
```

```python
import functools

import jax
import jax.numpy as jnp
from jax import lax
from jax.experimental import pallas as pl
from jax.experimental.pallas import tpu as pltpu
from jax.sharding import Mesh
from jax.sharding import PartitionSpec as P


grad_scale = 0.0625
lanes = 128
own_tile = 512
rest_tile = 1024
last_tile = 512
kernel_grant = 48 << 20
load_depth = 4
stage_grant = 1 << 20


smem_spec = pl.BlockSpec(memory_space=pltpu.SMEM)
vmem_spec = pl.BlockSpec(memory_space=pltpu.VMEM)
hbm_spec = pl.BlockSpec(memory_space=pltpu.HBM)
any_spec = pl.BlockSpec(memory_space=pl.ANY)


def contract(left, right, left_dim, right_dim):
    return lax.dot_general(
        left, right, (((left_dim,), (right_dim,)), ((), ())), preferred_element_type=jnp.float32
    )


def partner_of(group, step, groups):
    if groups & (groups - 1) == 0:
        return group ^ step
    return (group + step) % groups


def partner(group, step, groups, sign):
    if groups & (groups - 1) == 0:
        return group ^ step
    return lax.rem(group + sign * step + groups, groups)


def pack_kernel(repeats, groups, capacity, ids, counts, table, x_ref, cot_ref, *outs):
    all_ref, near_refs = outs[0], outs[1:]
    model_width = x_ref.shape[1]
    task_count = table.shape[0]
    own_repeat = lax.axis_index("rep")
    own_group = lax.axis_index("grp")
    row = lax.broadcasted_iota(jnp.int32, (capacity, lanes), 0)
    all_ids = ids[...].astype(jnp.float32)
    slot_row = lax.broadcasted_iota(jnp.int32, (capacity, all_ids.shape[1]), 0)
    place = lax.broadcasted_iota(jnp.int32, (capacity, all_ids.shape[1]), 1)
    for step in range(groups):
        group = partner(own_group, step, groups, 1)
        start = pl.multiple_of(group * capacity, capacity)
        live = counts[0, group]
        picked = jnp.where(place == slot_row + start, all_ids, 0.0)
        tags = jnp.sum(picked, axis=1, keepdims=True)
        tags = jnp.where(row < live, jnp.broadcast_to(tags, row.shape), task_count)
        rows = pl.ds(start, capacity)
        for hop in range(repeats):
            expert = lax.rem(own_repeat + hop, repeats) * groups + group
            block_refs = [all_ref.at[expert]]
            if hop == 0 and near_refs:
                block_refs.append(near_refs[step])
            gate = jnp.zeros((capacity, lanes), jnp.float32)
            for task in range(task_count):
                gate = jnp.where(tags == task, table[task, expert], gate)
            for ref in block_refs:
                ref[:, :model_width] = x_ref[rows, :]
            for column in range(0, model_width, lanes):
                part = cot_ref[rows, column : column + lanes].astype(jnp.float32) * gate
                part = part.astype(jnp.bfloat16)
                for ref in block_refs:
                    ref[:, model_width + column : model_width + column + lanes] = part


def pack_blocks(sizes, task_ids, group_counts, task_gate, inputs, cotangent):
    repeats, groups, halves, capacity = sizes
    width = 2 * inputs.shape[1]
    near_count = groups if halves > 1 else 0
    out_shape = [jax.ShapeDtypeStruct((repeats * groups, capacity, width), jnp.bfloat16)]
    out_shape += [jax.ShapeDtypeStruct((capacity, width), jnp.bfloat16)] * near_count
    outs = pl.pallas_call(
        functools.partial(pack_kernel, repeats, groups, capacity),
        out_shape=out_shape,
        in_specs=[vmem_spec, smem_spec, smem_spec, vmem_spec, vmem_spec],
        out_specs=[vmem_spec] * len(out_shape),
        name="pack_blocks",
    )(task_ids.reshape(1, -1), group_counts, task_gate, inputs, cotangent)
    return outs[0], outs[1:]


def weight_copies(tile, first_hbm, second_hbm, first_ref, second_ref, sems):
    copies = []
    for index in range(first_ref.shape[1] // tile):
        part = slice(index * tile, (index + 1) * tile)
        copies.append(
            (
                pltpu.make_async_copy(
                    first_hbm.at[:, part], first_ref.at[:, part], sems.at[2 * index]
                ),
                pltpu.make_async_copy(
                    second_hbm.at[part, :], second_ref.at[part, :], sems.at[2 * index + 1]
                ),
            )
        )
    for pair in copies[:load_depth]:
        start_pair(pair)
    return copies


def start_pair(pair):
    for copy in pair:
        copy.start()


def wait_pair(pair):
    for copy in pair:
        copy.wait()


def next_pair(copies, index):
    if index + load_depth < len(copies):
        start_pair(copies[index + load_depth])
    wait_pair(copies[index])


def weight_scratch(first_weight, second_weight, tile):
    return [
        pltpu.VMEM(first_weight.shape, first_weight.dtype),
        pltpu.VMEM(second_weight.shape, second_weight.dtype),
        pltpu.SemaphoreType.DMA((2 * first_weight.shape[1] // tile,)),
    ]


def hidden_chunk(x_rows, scaled_cot, first, second):
    pre_act = contract(x_rows, first, 1, 0)
    hidden_cot = contract(scaled_cot, second, 1, 1)
    sigmoid_act = 1.0 / (1.0 + jnp.exp(-pre_act))
    value = pre_act * sigmoid_act
    slope = sigmoid_act * (1.0 + pre_act - value)
    return value.astype(jnp.bfloat16), (hidden_cot * slope).astype(jnp.bfloat16)


def own_kernel(repeats, halves, rows_ref, first_hbm, second_hbm, *refs):
    act_out, pre_ref, x_ref, scaled_ref, grad_ref, far_ref = refs[:6]
    act_ref, total_ref, first_ref, second_ref, sems = refs[6:]
    row_count = rows_ref.shape[0]
    model_width, hidden_width = first_ref.shape
    copies = weight_copies(own_tile, first_hbm, second_hbm, first_ref, second_ref, sems)
    per_repeat = row_count // repeats
    own_repeat = lax.axis_index("rep")
    half = lax.axis_index("dp")
    for hop in range(1, repeats):
        source = lax.rem(own_repeat + hop, repeats)
        start = pl.multiple_of(source * per_repeat, per_repeat)
        far_ref[hop - 1] = rows_ref[pl.ds(start, per_repeat), :]
    first_rows = model_width // halves
    x_ref[...] = rows_ref[:, pl.ds(pl.multiple_of(half * first_rows, first_rows), first_rows)]
    scaled_ref[...] = rows_ref[:, model_width:]
    x_rows = rows_ref[:, :model_width]
    scaled_cot = rows_ref[:, model_width:]
    last = hidden_width // own_tile - 1
    for index in range(last + 1):
        columns = slice(index * own_tile, (index + 1) * own_tile)
        next_pair(copies, index)
        act, pre = hidden_chunk(x_rows, scaled_cot, first_ref[:, columns], second_ref[columns, :])
        act_ref[:, columns] = act
        pre_ref[:, columns] = pre
        if index == last:
            second_rows = hidden_width // halves
            begin = pl.multiple_of(half * second_rows, second_rows)
            act_out[...] = act_ref[:, pl.ds(begin, second_rows)]
        part = contract(pre, first_ref[:, columns], 1, 1)
        if index == 0:
            total_ref[...] = part
        elif index < last:
            total_ref[...] += part
        else:
            grad_ref[...] = (total_ref[...] + part).astype(jnp.bfloat16)


def own_parts(repeats, halves, rows, first_weight, second_weight):
    row_count, width = rows.shape
    model_width, hidden_width = first_weight.shape

    def shaped(*shape):
        return jax.ShapeDtypeStruct(shape, jnp.bfloat16)

    return pl.pallas_call(
        functools.partial(own_kernel, repeats, halves),
        out_shape=[
            shaped(row_count, hidden_width // halves),
            shaped(row_count, hidden_width),
            shaped(row_count, model_width // halves),
            shaped(row_count, model_width),
            shaped(row_count, model_width),
            shaped(repeats - 1, row_count // repeats, width),
        ],
        in_specs=[vmem_spec, any_spec, any_spec],
        out_specs=[vmem_spec] * 6,
        scratch_shapes=[
            pltpu.VMEM((row_count, hidden_width), jnp.bfloat16),
            pltpu.VMEM((row_count, model_width), jnp.float32),
            *weight_scratch(first_weight, second_weight, own_tile),
        ],
        compiler_params=pltpu.CompilerParams(vmem_limit_bytes=kernel_grant),
        cost_estimate=pl.CostEstimate(
            flops=6 * row_count * model_width * hidden_width,
            bytes_accessed=4 * model_width * hidden_width,
            transcendentals=0,
        ),
        name="own_parts",
    )(rows, first_weight, second_weight)


def stage_kernel(count, *refs):
    sems = refs[-1]
    copies = [
        pltpu.make_async_copy(refs[i], refs[count + i], sems.at[i]) for i in range(count)
    ]
    start_pair(copies)
    wait_pair(copies)


def stage(arrays):
    count = len(arrays)
    return pl.pallas_call(
        functools.partial(stage_kernel, count),
        out_shape=[jax.ShapeDtypeStruct(part.shape, part.dtype) for part in arrays],
        in_specs=[any_spec] * count,
        out_specs=[any_spec] * count,
        scratch_shapes=[pltpu.SemaphoreType.DMA((count,))],
        compiler_params=pltpu.CompilerParams(vmem_limit_bytes=stage_grant),
        name="stage",
    )(*arrays)


def rest_kernel(other_count, act_ref, pre_ref, x_ref, scaled_ref, *refs):
    other_refs = refs[:other_count]
    first_ref, second_ref, first_out, second_out = refs[other_count : other_count + 4]
    scratch = refs[other_count + 4 :]
    other, other_act, all_act, all_pre, scaled, left, first_buf, second_buf, sems = scratch
    own_count = act_ref.shape[0]
    model_width, _ = first_ref.shape
    first_tiles, first_rows, first_tile = first_buf.shape
    second_tiles, second_tile, _ = second_buf.shape
    half = lax.axis_index("dp")
    place = 0
    for ref in other_refs:
        other[place : place + ref.shape[0], :] = ref[...]
        place += ref.shape[0]
    x_begin = pl.multiple_of(half * first_rows, first_rows)
    left[:, :own_count] = x_ref[...].T
    left[:, own_count:] = other[:, pl.ds(x_begin, first_rows)].T
    scaled[:own_count, :] = scaled_ref[...]
    scaled[own_count:, :] = other[:, model_width:]
    all_act[:own_count, :] = act_ref[...]
    copies = []
    for tile in range(first_tiles):
        columns = slice(tile * first_tile, (tile + 1) * first_tile)
        act, pre = hidden_chunk(
            other[:, :model_width],
            other[:, model_width:],
            first_ref[:, columns],
            second_ref[columns, :],
        )
        other_act[:, columns] = act
        all_pre[:own_count, :] = pre_ref[:, columns]
        all_pre[own_count:, :] = pre
        first_buf[tile] = contract(left[...], all_pre[...], 1, 0) * grad_scale
        if copies:
            copies[-1].start()
        copies.append(
            pltpu.make_async_copy(first_buf.at[tile], first_out.at[:, columns], sems.at[tile])
        )
    second_rows = second_tiles * second_tile
    begin = pl.multiple_of(half * second_rows, second_rows)
    all_act[own_count:, :] = other_act[:, pl.ds(begin, second_rows)]
    for tile in range(second_tiles):
        rows = slice(tile * second_tile, (tile + 1) * second_tile)
        second_buf[tile] = contract(all_act[:, rows].T, scaled[...], 1, 0) * grad_scale
        copies[-1].start()
        copies.append(
            pltpu.make_async_copy(
                second_buf.at[tile], second_out.at[rows, :], sems.at[first_tiles + tile]
            )
        )
    copies[-1].start()
    for copy in copies:
        copy.wait()


def rest_parts(own, others, first_weight, second_weight):
    own_count, second_rows = own[0].shape
    first_rows = own[2].shape[1]
    width = others[0].shape[1]
    model_width, hidden_width = first_weight.shape
    other_rows = sum(part.shape[0] for part in others)
    first_tiles = hidden_width // rest_tile
    second_tiles = second_rows // last_tile
    row_count = own_count + other_rows
    flops = 4 * (row_count * first_rows + other_rows * model_width) * hidden_width
    return pl.pallas_call(
        functools.partial(rest_kernel, len(others)),
        out_shape=[
            jax.ShapeDtypeStruct((first_rows, hidden_width), jnp.float32),
            jax.ShapeDtypeStruct((second_rows, model_width), jnp.float32),
        ],
        in_specs=[vmem_spec] * (6 + len(others)),
        out_specs=[hbm_spec, hbm_spec],
        scratch_shapes=[
            pltpu.VMEM((other_rows, width), jnp.bfloat16),
            pltpu.VMEM((other_rows, hidden_width), jnp.bfloat16),
            pltpu.VMEM((row_count, second_rows), jnp.bfloat16),
            pltpu.VMEM((row_count, rest_tile), jnp.bfloat16),
            pltpu.VMEM((row_count, model_width), jnp.bfloat16),
            pltpu.VMEM((first_rows, row_count), jnp.bfloat16),
            pltpu.VMEM((first_tiles, first_rows, rest_tile), jnp.float32),
            pltpu.VMEM((second_tiles, last_tile, model_width), jnp.float32),
            pltpu.SemaphoreType.DMA((first_tiles + second_tiles,)),
        ],
        compiler_params=pltpu.CompilerParams(
            vmem_limit_bytes=min(60 << 20, (20 << 20) + row_count * (24 << 10))
        ),
        cost_estimate=pl.CostEstimate(
            flops=flops, bytes_accessed=8 * first_rows * hidden_width, transcendentals=0
        ),
        name="rest_parts",
    )(*own, *others, first_weight, second_weight)


def on_device(inputs, cotangent, task_ids, group_counts, task_gate, w_in, w_out):
    groups = group_counts.shape[1]
    model_width = inputs.shape[1]
    capacity = inputs.shape[0] // groups
    repeats = lax.axis_size("rep")
    halves = lax.axis_size("dp")
    first_weight = w_in[0]
    second_weight = w_out[0]
    outgoing, near = pack_blocks(
        (repeats, groups, halves, capacity), task_ids, group_counts, task_gate, inputs, cotangent
    )
    width = outgoing.shape[-1]

    def across(turn, step):
        pairs = []
        for source in range(groups * halves):
            group, half = divmod(source, halves)
            target = partner_of(group, step, groups) * halves + (half + turn) % halves
            pairs.append((source, target))
        return pairs

    own_rows = lax.all_to_all(outgoing, ("rep", "grp"), 0, 0)
    near_other = [
        lax.ppermute(near[step], ("grp", "dp"), across(turn, step))
        for turn in range(1, halves)
        for step in reversed(range(groups))
    ]
    own = own_rows.reshape(repeats * groups * capacity, width)
    *own_kept, row_grads, far_rows = own_parts(repeats, halves, own, first_weight, second_weight)
    far_other = []
    for hop in range(repeats - 1):
        for turn in range(1, halves):
            pairs = [(i, (i + turn) % halves) for i in range(halves)]
            far_other.append(lax.ppermute(far_rows[hop], "dp", pairs))
    returned = lax.all_to_all(
        row_grads.reshape(repeats * groups, capacity, model_width), ("rep", "grp"), 0, 0
    )
    *own_kept, first_weight, second_weight = stage([*own_kept, first_weight, second_weight])
    grad_first, grad_second = rest_parts(
        own_kept, near_other + far_other, first_weight, second_weight
    )
    input_home = jnp.sum(
        returned.reshape(repeats, groups * capacity, model_width).astype(jnp.float32), axis=0
    )
    return (input_home, grad_first[None], grad_second[None])


def solution(mesh):

    def step(inputs, cotangent, task_ids, group_counts, task_gate, w_in, w_out):
        groups = group_counts.shape[1]
        halves = mesh.shape["dp"]
        repeats = mesh.shape["blk"] // groups
        fine = Mesh(mesh.devices.reshape(repeats, groups, halves), ("rep", "grp", "dp"))
        rows = P(("rep", "grp", "dp"))
        expert = P(("rep", "grp"))
        split = P(("rep", "grp"), "dp")
        return jax.shard_map(
            on_device,
            mesh=fine,
            in_specs=(rows, rows, rows, rows, P(), expert, expert),
            out_specs=(rows, split, split),
            check_vma=False,
        )(inputs, cotangent, task_ids, group_counts, task_gate, w_in, w_out)

    return step
```
